32 devices in a mesh: dp: 1 (over z), tp: 4 (over y), cp: 8 (over x, core).
Axes of the slice: x: 4, y: 4, z: 1, core: 2. Of those that a mesh axis runs over, the one named last changes fastest.
The devices are a block of a 4x4x8 slice.
Arguments:
- hidden: bfloat16 [16, 64, 3072], P('dp')
- prefix_len: int32 [16], P('dp')
- k_cache: bfloat16 [16, 16384, 8, 128], P('dp', 'cp', 'tp')
- v_cache: bfloat16 [16, 16384, 8, 128], P('dp', 'cp', 'tp')
- attn_norm: bfloat16 [3072], replicated
- w_q: bfloat16 [3072, 3072], P(None, 'tp')
- w_k: bfloat16 [3072, 1024], P(None, 'tp')
- w_v: bfloat16 [3072, 1024], P(None, 'tp')
- w_o: bfloat16 [3072, 3072], P('tp')
- q_norm: bfloat16 [128], replicated
- k_norm: bfloat16 [128], replicated
Outputs:
- output 1: bfloat16 [16, 64, 3072], P('dp')
- output 2: bfloat16 [16, 64, 8, 128], P('dp', None, 'tp')
- output 3: bfloat16 [16, 64, 8, 128], P('dp', None, 'tp')
All inputs are finite; a program needn't handle non-finite values.
Results may differ from the reference program's by a relative error of at most 0.00825885.
Values sent between devices are 32-bit elements.
A program may use at most 768 MiB of HBM per device.

```python
import jax
import jax.numpy as jnp
from jax import lax

NUM_SEQ = 16
NEW_TOKENS = 64
CACHE_LEN = 16384
D_MODEL = 3072
N_HEADS = 24
KV_HEADS = 8
HEAD_DIM = 128


def rms_scale(tensor, norm_gain):
    mean_sq = jnp.mean(jnp.square(tensor), axis=-1, keepdims=True)
    return tensor * lax.rsqrt(mean_sq + 1e-6) * norm_gain


def rope_apply(tensor, positions):
    half_dim = HEAD_DIM // 2
    inv_freq = 1.0 / (1000000.0 ** (jnp.arange(half_dim, dtype=jnp.float32) * 2.0 / HEAD_DIM))
    angles = positions.astype(jnp.float32)[..., None] * inv_freq
    cos_t = jnp.cos(angles)[..., None, :]
    sin_t = jnp.sin(angles)[..., None, :]
    lead_half = tensor[..., :half_dim]
    tail_half = tensor[..., half_dim:]
    return jnp.concatenate([lead_half * cos_t - tail_half * sin_t, tail_half * cos_t + lead_half * sin_t], axis=-1)


def smooth_field(key, amplitude):
    n_freq = 4
    coords = (jnp.arange(CACHE_LEN, dtype=jnp.float32) + 0.5) / CACHE_LEN
    angles = jnp.pi * coords[:, None] * jnp.arange(1, n_freq + 1, dtype=jnp.float32)[None, :]
    cos_basis = jnp.concatenate([jnp.cos(angles), jnp.sin(angles)], axis=1)
    coeffs = jax.random.normal(key, (NUM_SEQ, 2 * n_freq, KV_HEADS, HEAD_DIM), jnp.float32) * (amplitude / n_freq ** 0.5)
    return jnp.einsum('pf,bfke->bpke', cos_basis, coeffs)


def setup_inputs(seed: int = 0, part: int = 0) -> dict:
    shared = jax.random.split(jax.random.key(seed), 8)
    part_keys = jax.random.split(jax.random.fold_in(jax.random.key(seed + 1), part), 8)
    cache_shape = (NUM_SEQ, CACHE_LEN, KV_HEADS, HEAD_DIM)
    len_draw = jax.random.randint(part_keys[1], (NUM_SEQ,), 0, CACHE_LEN + 1)
    full_at = jax.random.randint(part_keys[2], (), 0, NUM_SEQ)
    prefix_len = jnp.where(jnp.arange(NUM_SEQ) == full_at, CACHE_LEN, len_draw).astype(jnp.int32)
    k_cache = smooth_field(part_keys[3], 2.0) + 0.5 * jax.random.normal(part_keys[4], cache_shape, jnp.float32)
    v_cache = smooth_field(part_keys[5], 1.0) + 0.5 * jax.random.normal(part_keys[6], cache_shape, jnp.float32)
    q_width = N_HEADS * HEAD_DIM
    kv_width = KV_HEADS * HEAD_DIM
    return {
        'hidden': jax.random.normal(part_keys[0], (NUM_SEQ, NEW_TOKENS, D_MODEL), jnp.float32).astype(jnp.bfloat16),
        'prefix_len': prefix_len,
        'k_cache': k_cache.astype(jnp.bfloat16),
        'v_cache': v_cache.astype(jnp.bfloat16),
        'attn_norm': (1.0 + 0.4 * jax.random.normal(shared[0], (D_MODEL,), jnp.float32)).astype(jnp.bfloat16),
        'w_q': (jax.random.normal(shared[1], (D_MODEL, q_width), jnp.float32) * D_MODEL ** -0.5).astype(jnp.bfloat16),
        'w_k': (jax.random.normal(shared[2], (D_MODEL, kv_width), jnp.float32) * D_MODEL ** -0.5).astype(jnp.bfloat16),
        'w_v': (jax.random.normal(shared[3], (D_MODEL, kv_width), jnp.float32) * D_MODEL ** -0.5).astype(jnp.bfloat16),
        'w_o': (jax.random.normal(shared[4], (q_width, D_MODEL), jnp.float32) * q_width ** -0.5).astype(jnp.bfloat16),
        'q_norm': (1.0 + 0.4 * jax.random.normal(shared[5], (HEAD_DIM,), jnp.float32)).astype(jnp.bfloat16),
        'k_norm': (1.0 + 0.4 * jax.random.normal(shared[6], (HEAD_DIM,), jnp.float32)).astype(jnp.bfloat16),
    }


def reference(hidden, prefix_len, k_cache, v_cache, attn_norm, w_q, w_k, w_v, w_o, q_norm, k_norm):
    group_size = N_HEADS // KV_HEADS
    flat_rows = hidden.reshape(NUM_SEQ * NEW_TOKENS, D_MODEL)
    normed = rms_scale(flat_rows.astype(jnp.float32), attn_norm.astype(jnp.float32)).astype(jnp.bfloat16)
    q_lin = jnp.dot(normed, w_q, preferred_element_type=jnp.float32).astype(jnp.bfloat16)
    k_lin = jnp.dot(normed, w_k, preferred_element_type=jnp.float32).astype(jnp.bfloat16)
    v_lin = jnp.dot(normed, w_v, preferred_element_type=jnp.float32).astype(jnp.bfloat16)
    positions = prefix_len[:, None] + jnp.arange(NEW_TOKENS, dtype=jnp.int32)[None, :]
    q_heads = q_lin.reshape(NUM_SEQ, NEW_TOKENS, N_HEADS, HEAD_DIM).astype(jnp.float32)
    k_heads = k_lin.reshape(NUM_SEQ, NEW_TOKENS, KV_HEADS, HEAD_DIM).astype(jnp.float32)
    q_rot = rope_apply(rms_scale(q_heads, q_norm.astype(jnp.float32)), positions).astype(jnp.bfloat16)
    k_new = rope_apply(rms_scale(k_heads, k_norm.astype(jnp.float32)), positions).astype(jnp.bfloat16)
    v_new = v_lin.reshape(NUM_SEQ, NEW_TOKENS, KV_HEADS, HEAD_DIM)
    causal = jnp.arange(NEW_TOKENS)[:, None] >= jnp.arange(NEW_TOKENS)[None, :]
    score_scale = HEAD_DIM ** -0.5

    def one_sequence(operands):
        q_seq, k_seq, v_seq, kc_seq, vc_seq, seq_len = operands
        cache_ok = jnp.arange(CACHE_LEN) < seq_len
        key_mask = jnp.concatenate([jnp.broadcast_to(cache_ok[None, :], (NEW_TOKENS, CACHE_LEN)), causal], axis=1)

        def one_head_group(group_ops):
            q_grp, key_all, val_all = group_ops
            scores = jnp.einsum('cgd,kd->gck', q_grp.astype(jnp.float32), key_all.astype(jnp.float32)) * score_scale
            scores = jnp.where(key_mask[None], scores, -jnp.inf)
            prob_mat = jax.nn.softmax(scores, axis=-1)
            return jnp.einsum('gck,kd->cgd', prob_mat, val_all.astype(jnp.float32))

        key_all = jnp.concatenate([kc_seq, k_seq], axis=0).transpose(1, 0, 2)
        val_all = jnp.concatenate([vc_seq, v_seq], axis=0).transpose(1, 0, 2)
        q_grp = q_seq.reshape(NEW_TOKENS, KV_HEADS, group_size, HEAD_DIM).transpose(1, 0, 2, 3)
        out_grp = lax.map(one_head_group, (q_grp, key_all, val_all))
        return out_grp.transpose(1, 0, 2, 3).reshape(NEW_TOKENS, N_HEADS * HEAD_DIM)

    attn_seq = lax.map(one_sequence, (q_rot, k_new, v_new, k_cache, v_cache, prefix_len))
    attn_rows = attn_seq.reshape(NUM_SEQ * NEW_TOKENS, N_HEADS * HEAD_DIM).astype(jnp.bfloat16)
    block_out = flat_rows.astype(jnp.float32) + jnp.dot(attn_rows, w_o, preferred_element_type=jnp.float32)
    return block_out.astype(jnp.bfloat16).reshape(NUM_SEQ, NEW_TOKENS, D_MODEL), k_new, v_new
```

```python
import functools

import jax
import jax.numpy as jnp
from jax import lax
from jax.experimental import pallas as pl
from jax.experimental.pallas import tpu as pltpu
from jax.sharding import PartitionSpec as P

HEAD_DIM = 128
MASKED = -1e30
LOW = -3e38
EXP_SCALE = (HEAD_DIM ** -0.5) * 1.4426950408889634
WAVES = 2
STAT_ROWS = 8
MESH = pl.DeviceIdType.MESH
F32 = jnp.float32
BF16 = jnp.bfloat16


def rms_scale(tensor, norm_gain):
    mean_sq = jnp.mean(jnp.square(tensor), axis=-1, keepdims=True)
    return tensor * lax.rsqrt(mean_sq + 1e-6) * norm_gain


def rope_apply(tensor, positions):
    half_dim = HEAD_DIM // 2
    inv_freq = 1.0 / (1000000.0 ** (jnp.arange(half_dim, dtype=F32) * 2.0 / HEAD_DIM))
    angles = positions.astype(F32)[..., None] * inv_freq
    cos_t = jnp.cos(angles)[..., None, :]
    sin_t = jnp.sin(angles)[..., None, :]
    lead_half = tensor[..., :half_dim]
    tail_half = tensor[..., half_dim:]
    return jnp.concatenate([lead_half * cos_t - tail_half * sin_t, tail_half * cos_t + lead_half * sin_t], axis=-1)


def project_new(hidden, attn_norm, w_q, w_k, w_v, q_norm, k_norm, prefix_len):
    n_seq, n_new, d_model = hidden.shape
    kv_count = w_k.shape[1] // HEAD_DIM
    head_count = w_q.shape[1] // HEAD_DIM
    normed = rms_scale(hidden.astype(F32), attn_norm.astype(F32)).astype(BF16)
    q_lin = jnp.einsum('bce,ef->bcf', normed, w_q, preferred_element_type=F32).astype(BF16)
    k_lin = jnp.einsum('bce,ef->bcf', normed, w_k, preferred_element_type=F32).astype(BF16)
    v_lin = jnp.einsum('bce,ef->bcf', normed, w_v, preferred_element_type=F32).astype(BF16)
    positions = prefix_len[:, None] + jnp.arange(n_new, dtype=jnp.int32)[None, :]
    q_heads = q_lin.reshape(n_seq, n_new, head_count, HEAD_DIM).astype(F32)
    k_heads = k_lin.reshape(n_seq, n_new, kv_count, HEAD_DIM).astype(F32)
    q_rot = rope_apply(rms_scale(q_heads, q_norm.astype(F32)), positions).astype(BF16)
    k_new = rope_apply(rms_scale(k_heads, k_norm.astype(F32)), positions).astype(BF16)
    return q_rot.reshape(n_seq, n_new, head_count * HEAD_DIM), k_new.reshape(n_seq, n_new, kv_count * HEAD_DIM), v_lin


def block_diag(pair):
    zero = jnp.zeros((pair.shape[0], HEAD_DIM), pair.dtype)
    top = jnp.concatenate([pair[:, :HEAD_DIM], zero], axis=1)
    low = jnp.concatenate([zero, pair[:, HEAD_DIM:]], axis=1)
    return jnp.concatenate([top, low], axis=0)


def dot_nt(a, b):
    return lax.dot_general(a, b, (((1,), (1,)), ((), ())), preferred_element_type=F32)


def attend_seq(q_tok, k_ref, v_ref, k_own, v_own, limit, own_on, score_ref, even_ref, odd_ref, write_out):
    n_new = q_tok.shape[0]
    group = q_tok.shape[1] // (2 * HEAD_DIM)
    rows = group * n_new
    n_keys = k_ref.shape[0]
    chunk = even_ref.shape[0]
    q_ext = jnp.concatenate([
        jnp.concatenate([q_tok[:, g * HEAD_DIM:(g + 1) * HEAD_DIM], q_tok[:, (group + g) * HEAD_DIM:(group + g + 1) * HEAD_DIM]], axis=1)
        for g in range(group)], axis=0)
    lane = lax.broadcasted_iota(jnp.int32, (rows, HEAD_DIM), 1)
    is_even = lane % 2 == 0
    key_lane = lax.broadcasted_iota(jnp.int32, (1, chunk), 1)
    run_max = jnp.full((rows, HEAD_DIM), MASKED, F32)
    for start in range(0, n_keys, chunk):
        keys = k_ref[pl.ds(start, chunk), :]
        keys_ext = jnp.concatenate([keys * even_ref[...], keys * odd_ref[...]], axis=1)
        scores = dot_nt(q_ext, keys_ext)
        scores = jnp.where(key_lane < 2 * limit - start, scores, MASKED)
        score_ref[:, pl.ds(start, chunk)] = scores
        for block in range(0, chunk, HEAD_DIM):
            run_max = jnp.maximum(run_max, scores[:, block:block + HEAD_DIM])
    s_own = dot_nt(q_ext, block_diag(k_own))
    own_row = lax.broadcasted_iota(jnp.int32, (rows, 2 * n_new), 0) % n_new
    own_lane = lax.broadcasted_iota(jnp.int32, (rows, 2 * n_new), 1)
    own_first = own_lane < n_new
    own_key = jnp.where(own_first, own_lane, own_lane - n_new)
    s_own = jnp.where((own_key <= own_row) & own_on, s_own, MASKED)
    max_0 = jnp.maximum(jnp.max(jnp.where(is_even, run_max, LOW), axis=1, keepdims=True),
                        jnp.max(jnp.where(own_first, s_own, LOW), axis=1, keepdims=True))
    max_1 = jnp.maximum(jnp.max(jnp.where(is_even, LOW, run_max), axis=1, keepdims=True),
                        jnp.max(jnp.where(own_first, LOW, s_own), axis=1, keepdims=True))
    max_lane = jnp.where(is_even, max_0, max_1)
    p_own = jnp.exp2((s_own - jnp.where(own_first, max_0, max_1)) * EXP_SCALE)
    acc = jnp.dot(p_own.astype(BF16), block_diag(v_own), preferred_element_type=F32)
    run_sum = jnp.zeros((rows, HEAD_DIM), F32)
    for start in range(0, n_keys, chunk):
        probs = []
        for block in range(start, start + chunk, HEAD_DIM):
            p_blk = jnp.exp2((score_ref[:, pl.ds(block, HEAD_DIM)] - max_lane) * EXP_SCALE)
            run_sum = run_sum + p_blk
            probs.append(p_blk.astype(BF16))
        vals = v_ref[pl.ds(start, chunk), :]
        vals_ext = jnp.concatenate([vals * even_ref[...], vals * odd_ref[...]], axis=1)
        acc = acc + jnp.dot(jnp.concatenate(probs, axis=1), vals_ext, preferred_element_type=F32)
    sum_0 = jnp.sum(jnp.where(is_even, run_sum, 0.0) + jnp.where(own_first, p_own, 0.0), axis=1, keepdims=True)
    sum_1 = jnp.sum(jnp.where(is_even, 0.0, run_sum) + jnp.where(own_first, 0.0, p_own), axis=1, keepdims=True)
    stat = jnp.where(lane == 0, max_0, jnp.where(lane == 1, max_1, jnp.where(lane == 2, sum_0, sum_1)))
    stat = jnp.concatenate([stat, jnp.zeros((2 * HEAD_DIM - rows, HEAD_DIM), F32)], axis=0)
    write_out(acc, stat.T[:STAT_ROWS])


def attend_kernel(len_ref, q_ref, kn_ref, vn_ref, k_hbm, v_hbm, out_ref, k_buf, v_buf, score_ref, even_ref, odd_ref, k_sem, v_sem):
    n_seq, n_keys = k_hbm.shape[0], k_hbm.shape[1]
    per_wave = n_seq // WAVES
    cp_index = lax.axis_index('cp')
    row = lax.broadcasted_iota(jnp.int32, even_ref.shape, 0)
    odd = (row % 2).astype(F32)
    odd_ref[...] = odd.astype(BF16)
    even_ref[...] = (1.0 - odd).astype(BF16)

    def seq_of(i):
        return (i // per_wave) * per_wave + 2 * (i % (per_wave // 2)) + (i % per_wave) // (per_wave // 2)

    def copies(i, slot):
        b = seq_of(i)
        return (pltpu.make_async_copy(k_hbm.at[b], k_buf.at[slot], k_sem.at[slot]),
                pltpu.make_async_copy(v_hbm.at[b], v_buf.at[slot], v_sem.at[slot]))

    for cp in copies(0, 0):
        cp.start()

    def step(i, carry):
        slot = i % 2
        b = seq_of(i)

        @pl.when(i + 1 < n_seq)
        def _():
            for cp in copies(i + 1, 1 - slot):
                cp.start()
        for cp in copies(i, slot):
            cp.wait()
        limit = len_ref[b] - cp_index * (n_keys // 2)

        def write_out(acc, stat):
            rows = acc.shape[0]
            out_ref[i, pl.ds(0, rows), :] = acc
            out_ref[i, pl.ds(rows, STAT_ROWS), :] = stat
        attend_seq(q_ref[b], k_buf.at[slot], v_buf.at[slot], kn_ref[b], vn_ref[b], limit, cp_index == 0, score_ref, even_ref, odd_ref, write_out)
        return carry
    lax.fori_loop(0, n_seq, step, 0)


def attend(prefix_len, q_tok, k_new, v_new, k_cache, v_cache):
    n_seq, n_new, q_width = q_tok.shape
    n_keys = k_cache.shape[1]
    rows = n_new * q_width // (2 * HEAD_DIM)
    chunk = min(512, n_keys)
    vmem = pl.BlockSpec(memory_space=pltpu.VMEM)
    hbm = pl.BlockSpec(memory_space=pl.ANY)
    return pl.pallas_call(
        attend_kernel,
        out_shape=jax.ShapeDtypeStruct((n_seq, rows + STAT_ROWS, 2 * HEAD_DIM), F32),
        in_specs=[pl.BlockSpec(memory_space=pltpu.SMEM), vmem, vmem, vmem, hbm, hbm],
        out_specs=vmem,
        scratch_shapes=[pltpu.VMEM((2, n_keys, HEAD_DIM), BF16), pltpu.VMEM((2, n_keys, HEAD_DIM), BF16),
                        pltpu.VMEM((rows, n_keys), F32), pltpu.VMEM((chunk, HEAD_DIM), BF16), pltpu.VMEM((chunk, HEAD_DIM), BF16),
                        pltpu.SemaphoreType.DMA((2,)), pltpu.SemaphoreType.DMA((2,))],
        compiler_params=pltpu.CompilerParams(vmem_limit_bytes=48 * 1024 * 1024),
        name='attend',
    )(prefix_len, q_tok, k_new, v_new, k_cache, v_cache)


def merge_units(units, rows, normalise):
    stats = [u[rows:rows + STAT_ROWS] for u in units]
    peak = functools.reduce(jnp.maximum, [s[0:2] for s in stats])
    facs = [jnp.exp2((s[0:2] - peak) * EXP_SCALE) for s in stats]
    total = functools.reduce(jnp.add, [s[2:4] * f for s, f in zip(stats, facs)])
    if normalise:
        facs = [f / total for f in facs]
    table = jnp.concatenate(facs, axis=0)
    table = jnp.concatenate([table, jnp.zeros((HEAD_DIM - table.shape[0], table.shape[1]), F32)], axis=0).T
    heads = []
    for h in range(2):
        parts = [u[:rows, h * HEAD_DIM:(h + 1) * HEAD_DIM] * table[:rows, 2 * i + h:2 * i + h + 1] for i, u in enumerate(units)]
        heads.append(functools.reduce(jnp.add, parts))
    stat = jnp.concatenate([peak, total, jnp.zeros((STAT_ROWS - 4, total.shape[1]), F32)], axis=0)
    return jnp.concatenate(heads, axis=1), stat


class Exchange:
    def __init__(self, wave, refs, n_cp, n_tp):
        self.w = wave
        self.r = refs
        self.n_x = n_cp // 2
        self.n_cp = n_cp
        self.n_tp = n_tp
        self.cp = lax.axis_index('cp')
        self.tp = lax.axis_index('tp')
        self.x = self.cp // 2
        self.core = self.cp % 2
        self.pending = []

    def cp_at(self, dx):
        return lax.rem(self.cp + 2 * dx + self.n_cp, self.n_cp)

    def tp_at(self, dy):
        return lax.rem(self.tp + dy + self.n_tp, self.n_tp)

    def send(self, src, dst, recv_sem, cp=None, tp=None):
        self.r['count'][0] += 1
        where = {}
        if cp is not None:
            where['cp'] = cp
        if tp is not None:
            where['tp'] = tp
        copy = pltpu.make_async_remote_copy(src_ref=src, dst_ref=dst, send_sem=self.r['send'].at[self.r['count'][0] - 1], recv_sem=recv_sem,
                                            device_id=where, device_id_type=MESH)
        copy.start()
        self.pending.append(copy)

    def wait(self, dst, recv_sem):
        pltpu.make_async_remote_copy(src_ref=dst, dst_ref=dst, send_sem=self.r['send'].at[0], recv_sem=recv_sem,
                                     device_id={'cp': self.cp}, device_id_type=MESH).wait_recv()

    @property
    def partner(self):
        return self.cp + 1 - 2 * self.core

    def pair_send(self):
        r, w = self.r, self.w
        self.send(r['sums'].at[w, 1 - self.core], r['pair'].at[w], r['pair_sem'].at[w], cp=self.partner)

    def pair_merge(self):
        r, w, rows = self.r, self.w, self.r['rows']
        self.wait(r['pair'].at[w], r['pair_sem'].at[w])
        for d in (2, 1, 3, 0):
            ox = lax.rem(self.x + d, self.n_x)
            merged, stat = merge_units([r['pair'][w, ox], r['sums'][w, self.core, ox]], rows, False)
            r['pair'][w, ox, pl.ds(0, rows), :] = merged
            r['pair'][w, ox, pl.ds(rows, STAT_ROWS), :] = stat
            if d:
                self.send(r['pair'].at[w, ox], r['xin'].at[w, d - 1], r['xin_sem'].at[w, d - 1], cp=self.cp_at(d))

    def project_out(self):
        r, w, rows = self.r, self.w, self.r['rows']
        for d in range(1, self.n_x):
            self.wait(r['xin'].at[w, d - 1], r['xin_sem'].at[w, d - 1])
        units = [r['pair'][w, self.x]] + [r['xin'][w, d - 1] for d in range(1, self.n_x)]
        attn, _ = merge_units(units, rows, True)
        attn = attn.astype(BF16)
        n_new = r['n_new']
        group = rows // n_new
        lhs = jnp.concatenate([attn[g * n_new:(g + 1) * n_new, k * HEAD_DIM:(k + 1) * HEAD_DIM] for k in range(2) for g in range(group)], axis=1)
        width = r['wo'].shape[1] // self.n_tp
        for d in (2, 1, 3, 0):
            oy = lax.rem(self.tp + d, self.n_tp)
            for part in range(0, width, 256):
                cols = pl.ds(pl.multiple_of(oy * width + part, 128), 256)
                r['yout'][w, oy, :, pl.ds(part, 256)] = jnp.dot(lhs, r['wo'][:, cols], preferred_element_type=F32)
            if d:
                self.send(r['yout'].at[w, oy], r['yin'].at[w, d - 1], r['yin_sem'].at[w, d - 1], tp=self.tp_at(d))

    def finish_rows(self):
        r, w = self.r, self.w
        for d in range(1, self.n_tp):
            self.wait(r['yin'].at[w, d - 1], r['yin_sem'].at[w, d - 1])
        width = r['wo'].shape[1] // self.n_tp
        seq = w * self.n_cp + self.cp
        total = r['yout'][w, self.tp]
        for d in range(1, self.n_tp):
            total = total + r['yin'][w, d - 1]
        cols = pl.ds(pl.multiple_of(self.tp * width, 128), width)
        total = total + r['x'][seq, :, cols].astype(F32)
        r['gather'][w, self.cp, self.tp] = total.astype(BF16).astype(F32)

    def unit(self, half, rx, ry, sub=None):
        n_half = self.r['n_new'] // 2
        start, size = half * n_half, n_half
        if sub is not None:
            start, size = start + sub * (n_half // 2), n_half // 2
        return self.r['gather'].at[self.w, self.cp_at(rx), self.tp_at(ry), pl.ds(start, size), :]

    def hop(self, half, rx, ry, axis, step, sub=None):
        ref = self.unit(half, rx, ry, sub)
        tx, ty = (rx - step) % self.n_x, ry
        if axis == 'y':
            tx, ty = rx, (ry - step) % self.n_tp
        sem = self.r['gather_sem'].at[self.w, half, tx, ty, sub or 0]
        if axis == 'x':
            self.send(ref, ref, sem, cp=self.cp_at(step))
        else:
            self.send(ref, ref, sem, tp=self.tp_at(step))

    def arrive(self, half, rx, ry, sub=None):
        self.wait(self.unit(half, rx, ry, sub), self.r['gather_sem'].at[self.w, half, rx, ry, sub or 0])

    def share(self, half, rx, ry):
        ref = self.unit(half, rx, ry)
        self.send(ref, ref, self.r['share_sem'].at[self.w, half, rx, ry], cp=self.partner)

    def first(self, half):
        return ('x', 'y') if half == 0 else ('y', 'x')

    def at(self, half, a, b):
        return (a, b) if half == 0 else (b, a)

    def gather_start(self):
        for half in (0, 1):
            one, two = self.first(half)
            for axis in (one, two):
                for step in (1, -1):
                    self.hop(half, 0, 0, axis, step)
        for half in (0, 1):
            self.share(half, 0, 0)

    def gather_first(self):
        for a, step in ((3, 1), (1, -1)):
            for half in (0, 1):
                one, two = self.first(half)
                rx, ry = self.at(half, a, 0)
                self.arrive(half, rx, ry)
                self.hop(half, rx, ry, one, step, sub=0 if step == 1 else 1)
                self.hop(half, rx, ry, two, 1)
                self.hop(half, rx, ry, two, -1)
                self.share(half, rx, ry)

    def gather_opposite(self):
        for half in (0, 1):
            one, two = self.first(half)
            rx, ry = self.at(half, 2, 0)
            self.arrive(half, rx, ry, 0)
            self.arrive(half, rx, ry, 1)
            self.hop(half, rx, ry, two, 1)
            self.hop(half, rx, ry, two, -1)
            self.share(half, rx, ry)

    def gather_second(self):
        for a in (0, 3, 1, 2):
            for b, step in ((3, 1), (1, -1)):
                for half in (0, 1):
                    one, two = self.first(half)
                    rx, ry = self.at(half, a, b)
                    self.arrive(half, rx, ry)
                    self.hop(half, rx, ry, two, step, sub=0 if step == 1 else 1)
                    self.share(half, rx, ry)

    def gather_last(self):
        for a in (0, 3, 1, 2):
            for half in (0, 1):
                rx, ry = self.at(half, a, 2)
                self.arrive(half, rx, ry, 0)
                self.arrive(half, rx, ry, 1)
                self.share(half, rx, ry)

    def gather_shared(self):
        for half in (0, 1):
            for rx in range(self.n_x):
                for ry in range(self.n_tp):
                    n_half = self.r['n_new'] // 2
                    cp = self.cp_at(rx) + 1 - 2 * self.core
                    ref = self.r['gather'].at[self.w, cp, self.tp_at(ry), pl.ds(half * n_half, n_half), :]
                    self.wait(ref, self.r['share_sem'].at[self.w, half, rx, ry])

    def write_rows(self):
        r, w = self.r, self.w
        width = r['wo'].shape[1] // self.n_tp

        def body(s, carry):
            for ty in range(self.n_tp):
                r['stage'][s, :, pl.ds(ty * width, width)] = r['gather'][w, s, ty].astype(BF16)
            pltpu.make_async_copy(r['stage'].at[s], r['out'].at[w * self.n_cp + s], r['out_sem'].at[w]).start()
            return carry
        if w:
            pltpu.make_async_copy(r['stage'], r['out'].at[pl.ds((w - 1) * self.n_cp, self.n_cp)], r['out_sem'].at[w - 1]).wait()
        lax.fori_loop(0, self.n_cp, body, 0)
        if w == WAVES - 1:
            pltpu.make_async_copy(r['stage'], r['out'].at[pl.ds(w * self.n_cp, self.n_cp)], r['out_sem'].at[w]).wait()


def entry_barrier(n_cp, n_tp):
    cp, tp = lax.axis_index('cp'), lax.axis_index('tp')
    barrier = pltpu.get_barrier_semaphore()
    peers = [{'cp': cp + 1 - 2 * (cp % 2)}]
    peers += [{'cp': lax.rem(cp + 2 * d, n_cp)} for d in range(1, n_cp // 2)]
    peers += [{'tp': lax.rem(tp + d, n_tp)} for d in range(1, n_tp)]
    for peer in peers:
        pl.semaphore_signal(barrier, inc=1, device_id=peer, device_id_type=MESH)
    pl.semaphore_wait(barrier, len(peers))


def exchange_kernel(n_cp, n_tp, n_new, sums_ref, x_ref, wo_ref, out_ref, pair, xin, yout, yin, gather, stage,
                    send_sem, pair_sem, xin_sem, yin_sem, gather_sem, share_sem, out_sem):
    entry_barrier(n_cp, n_tp)
    refs = {'sums': sums_ref, 'x': x_ref, 'wo': wo_ref, 'out': out_ref, 'pair': pair, 'xin': xin, 'yout': yout, 'yin': yin,
            'gather': gather, 'stage': stage, 'send': send_sem, 'pair_sem': pair_sem, 'xin_sem': xin_sem, 'yin_sem': yin_sem,
            'gather_sem': gather_sem, 'share_sem': share_sem, 'out_sem': out_sem, 'n_new': n_new, 'rows': sums_ref.shape[3] - STAT_ROWS,
            'count': [0]}
    waves = [Exchange(w, refs, n_cp, n_tp) for w in range(WAVES)]
    for name in ('pair_send', 'pair_merge', 'project_out', 'finish_rows+gather_start', 'gather_first', 'gather_opposite', 'gather_second',
                 'gather_last', 'gather_shared+write_rows'):
        for wave in waves:
            for part in name.split('+'):
                getattr(wave, part)()
    for wave in waves:
        for copy in wave.pending:
            copy.wait_send()


def exchange(sums, hidden, w_o, n_cp, n_tp):
    n_seq, n_new, d_model = hidden.shape
    unit_rows, unit_lanes = sums.shape[1:]
    n_x = n_cp // 2
    width = d_model // n_tp
    vmem = pl.BlockSpec(memory_space=pltpu.VMEM)
    n_send = WAVES * (1 + (n_x - 1) + (n_tp - 1) + 40 + 32)
    return pl.pallas_call(
        functools.partial(exchange_kernel, n_cp, n_tp, n_new),
        out_shape=jax.ShapeDtypeStruct((n_seq, n_new, d_model), BF16),
        in_specs=[vmem, vmem, vmem],
        out_specs=pl.BlockSpec(memory_space=pl.ANY),
        scratch_shapes=[
            pltpu.VMEM((WAVES, n_x, unit_rows, unit_lanes), F32),
            pltpu.VMEM((WAVES, n_x - 1, unit_rows, unit_lanes), F32),
            pltpu.VMEM((WAVES, n_tp, n_new, width), F32),
            pltpu.VMEM((WAVES, n_tp - 1, n_new, width), F32),
            pltpu.VMEM((WAVES, n_cp, n_tp, n_new, width), F32),
            pltpu.VMEM((n_cp, n_new, d_model), BF16),
            pltpu.SemaphoreType.DMA((n_send,)),
            pltpu.SemaphoreType.DMA((WAVES,)),
            pltpu.SemaphoreType.DMA((WAVES, n_x - 1)),
            pltpu.SemaphoreType.DMA((WAVES, n_tp - 1)),
            pltpu.SemaphoreType.DMA((WAVES, 2, n_x, n_tp, 2)),
            pltpu.SemaphoreType.DMA((WAVES, 2, n_x, n_tp)),
            pltpu.SemaphoreType.DMA((WAVES,)),
        ],
        compiler_params=pltpu.CompilerParams(collective_id=0, has_side_effects=True, vmem_limit_bytes=60 * 1024 * 1024),
        name='exchange',
    )(sums.reshape(WAVES, 2, n_x, unit_rows, unit_lanes), hidden, w_o)


def solution(mesh):
    n_cp, n_tp = mesh.shape['cp'], mesh.shape['tp']

    def per_device(hidden, prefix_len, k_cache, v_cache, attn_norm, w_q, w_k, w_v, w_o, q_norm, k_norm):
        n_seq, n_new, _ = hidden.shape
        slots = k_cache.shape[1]
        q_tok, k_new, v_new = project_new(hidden, attn_norm, w_q, w_k, w_v, q_norm, k_norm, prefix_len)
        sums = attend(prefix_len, q_tok, k_new, v_new, k_cache.reshape(n_seq, slots * 2, HEAD_DIM), v_cache.reshape(n_seq, slots * 2, HEAD_DIM))
        block_out = exchange(sums, hidden, w_o, n_cp, n_tp)
        return block_out, k_new.reshape(n_seq, n_new, 2, HEAD_DIM), v_new.reshape(n_seq, n_new, 2, HEAD_DIM)

    cache_spec = P('dp', 'cp', 'tp', None)
    arg_specs = (P('dp', None, None), P('dp'), cache_spec, cache_spec, P(None), P(None, 'tp'), P(None, 'tp'), P(None, 'tp'), P('tp', None), P(None), P(None))
    out_specs = (P('dp', None, None), P('dp', None, 'tp', None), P('dp', None, 'tp', None))
    return jax.shard_map(per_device, mesh=mesh, in_specs=arg_specs, out_specs=out_specs, check_vma=False)
```

```python
import functools

import jax
import jax.numpy as jnp
from jax import lax
from jax.experimental import pallas as pl
from jax.experimental.pallas import tpu as pltpu
from jax.sharding import PartitionSpec as P

HEAD_DIM = 128
MASKED = -1e30
LOW = -3e38
EXP_SCALE = (HEAD_DIM ** -0.5) * 1.4426950408889634
WAVE_SEQS = 4
STAT_ROWS = 8
MESH = pl.DeviceIdType.MESH
F32 = jnp.float32
BF16 = jnp.bfloat16


def rope_tables(prefix_len, n_new):
    half_dim = HEAD_DIM // 2
    positions = prefix_len[:, None] + jnp.arange(n_new, dtype=jnp.int32)[None, :]
    inv_freq = 1.0 / (1000000.0 ** (jnp.arange(half_dim, dtype=F32) * 2.0 / HEAD_DIM))
    angles = positions.astype(F32)[..., None] * inv_freq
    cos_t, sin_t = jnp.cos(angles), jnp.sin(angles)
    return jnp.concatenate([cos_t, cos_t, -sin_t, sin_t], axis=-1).reshape(-1, 2 * HEAD_DIM)


def block_diag(pair):
    zero = jnp.zeros((pair.shape[0], HEAD_DIM), pair.dtype)
    top = jnp.concatenate([pair[:, :HEAD_DIM], zero], axis=1)
    low = jnp.concatenate([zero, pair[:, HEAD_DIM:]], axis=1)
    return jnp.concatenate([top, low], axis=0)


def dot_nt(a, b):
    return lax.dot_general(a, b, (((1,), (1,)), ((), ())), preferred_element_type=F32)


def attend_seq(q_tok, k_ref, v_ref, k_own, v_own, limit, own_on, score_ref, even_ref, odd_ref):
    n_new = q_tok.shape[0]
    n_half = n_new // 2
    group = q_tok.shape[1] // (2 * HEAD_DIM)
    rows = group * n_new
    n_keys = k_ref.shape[0]
    chunk = even_ref.shape[0]
    q_ext = jnp.concatenate([
        jnp.concatenate([q_tok[h * n_half:(h + 1) * n_half, g * HEAD_DIM:(g + 1) * HEAD_DIM],
                         q_tok[h * n_half:(h + 1) * n_half, (group + g) * HEAD_DIM:(group + g + 1) * HEAD_DIM]], axis=1)
        for h in range(2) for g in range(group)], axis=0)
    lane = lax.broadcasted_iota(jnp.int32, (rows, HEAD_DIM), 1)
    is_even = lane % 2 == 0
    key_lane = lax.broadcasted_iota(jnp.int32, (1, chunk), 1)
    run_max = jnp.full((rows, HEAD_DIM), MASKED, F32)
    for start in range(0, n_keys, chunk):
        keys = k_ref[pl.ds(start, chunk), :]
        keys_ext = jnp.concatenate([keys * even_ref[...], keys * odd_ref[...]], axis=1)
        scores = dot_nt(q_ext, keys_ext)
        scores = jnp.where(key_lane < 2 * limit - start, scores, MASKED)
        score_ref[:, pl.ds(start, chunk)] = scores
        for block in range(0, chunk, HEAD_DIM):
            run_max = jnp.maximum(run_max, scores[:, block:block + HEAD_DIM])
    s_own = dot_nt(q_ext, block_diag(k_own))
    row = lax.broadcasted_iota(jnp.int32, (rows, 2 * n_new), 0)
    own_row = jnp.where(row < rows // 2, row, row + n_half) % n_half + jnp.where(row < rows // 2, 0, n_half)
    own_lane = lax.broadcasted_iota(jnp.int32, (rows, 2 * n_new), 1)
    own_first = own_lane < n_new
    own_key = jnp.where(own_first, own_lane, own_lane - n_new)
    s_own = jnp.where((own_key <= own_row) & own_on, s_own, MASKED)
    max_0 = jnp.maximum(jnp.max(jnp.where(is_even, run_max, LOW), axis=1, keepdims=True),
                        jnp.max(jnp.where(own_first, s_own, LOW), axis=1, keepdims=True))
    max_1 = jnp.maximum(jnp.max(jnp.where(is_even, LOW, run_max), axis=1, keepdims=True),
                        jnp.max(jnp.where(own_first, LOW, s_own), axis=1, keepdims=True))
    max_lane = jnp.where(is_even, max_0, max_1)
    p_own = jnp.exp2((s_own - jnp.where(own_first, max_0, max_1)) * EXP_SCALE)
    acc = jnp.dot(p_own.astype(BF16), block_diag(v_own), preferred_element_type=F32)
    run_sum = jnp.zeros((rows, HEAD_DIM), F32)
    for start in range(0, n_keys, chunk):
        probs = []
        for block in range(start, start + chunk, HEAD_DIM):
            p_blk = jnp.exp2((score_ref[:, pl.ds(block, HEAD_DIM)] - max_lane) * EXP_SCALE)
            run_sum = run_sum + p_blk
            probs.append(p_blk.astype(BF16))
        vals = v_ref[pl.ds(start, chunk), :]
        vals_ext = jnp.concatenate([vals * even_ref[...], vals * odd_ref[...]], axis=1)
        acc = acc + jnp.dot(jnp.concatenate(probs, axis=1), vals_ext, preferred_element_type=F32)
    sum_0 = jnp.sum(jnp.where(is_even, run_sum, 0.0) + jnp.where(own_first, p_own, 0.0), axis=1, keepdims=True)
    sum_1 = jnp.sum(jnp.where(is_even, 0.0, run_sum) + jnp.where(own_first, 0.0, p_own), axis=1, keepdims=True)
    stat = jnp.where(lane == 0, max_0, jnp.where(lane == 1, max_1, jnp.where(lane == 2, sum_0, sum_1)))
    pad = jnp.zeros((HEAD_DIM - rows // 2, HEAD_DIM), F32)
    stat = jnp.concatenate([stat[:rows // 2], pad, stat[rows // 2:], pad], axis=0)
    return acc, stat.T[:STAT_ROWS]


def merge_units(units, rows, normalise):
    stats = [u[rows:rows + STAT_ROWS, :HEAD_DIM] for u in units]
    peak = functools.reduce(jnp.maximum, [s[0:2] for s in stats])
    facs = [jnp.exp2((s[0:2] - peak) * EXP_SCALE) for s in stats]
    total = functools.reduce(jnp.add, [s[2:4] * f for s, f in zip(stats, facs)])
    if normalise:
        facs = [f / total for f in facs]
    table = jnp.concatenate(facs, axis=0)
    table = jnp.concatenate([table, jnp.zeros((HEAD_DIM - table.shape[0], table.shape[1]), F32)], axis=0).T
    heads = []
    for h in range(2):
        parts = [u[:rows, h * HEAD_DIM:(h + 1) * HEAD_DIM] * table[:rows, 2 * i + h:2 * i + h + 1] for i, u in enumerate(units)]
        heads.append(functools.reduce(jnp.add, parts))
    stat = jnp.concatenate([peak, total, jnp.zeros((STAT_ROWS - 4, total.shape[1]), F32)], axis=0)
    return jnp.concatenate(heads, axis=1), stat


class Exchange:
    def __init__(self, wave, refs, n_cp, n_tp):
        self.w = wave
        self.r = refs
        self.n_x = n_cp // 2
        self.n_cp = n_cp
        self.n_tp = n_tp
        self.cp = lax.axis_index('cp')
        self.tp = lax.axis_index('tp')
        self.x = self.cp // 2
        self.core = self.cp % 2

    def cp_at(self, dx):
        return lax.rem(self.cp + 2 * dx + self.n_cp, self.n_cp)

    def tp_at(self, dy):
        return lax.rem(self.tp + dy + self.n_tp, self.n_tp)

    def send(self, src, dst, recv_sem, cp=None, tp=None):
        where = {}
        if cp is not None:
            where['cp'] = cp
        if tp is not None:
            where['tp'] = tp
        sent = self.r['sent']
        copy = pltpu.make_async_remote_copy(src_ref=src, dst_ref=dst, send_sem=self.r['send'].at[self.w, len(sent)], recv_sem=recv_sem,
                                            device_id=where, device_id_type=MESH)
        copy.start()
        sent.append(src.shape)

    def wait(self, dst, recv_sem):
        pltpu.make_async_remote_copy(src_ref=dst, dst_ref=dst, send_sem=self.r['send'].at[0, 0], recv_sem=recv_sem,
                                     device_id={'cp': self.cp}, device_id_type=MESH).wait_recv()

    def wait_sends(self):
        for k, shape in enumerate(self.r['sent']):
            name = 'pair' if len(shape) == 3 else 'xin' if shape[0] == self.r['pair'].shape[2] else 'gather'
            ref = {'pair': lambda: self.r['pair'].at[self.w], 'xin': lambda: self.r['xin'].at[self.w, 0],
                   'gather': lambda: self.r['gather'].at[self.w, 0, 0, pl.ds(0, shape[0]), :]}[name]()
            pltpu.make_async_remote_copy(src_ref=ref, dst_ref=ref, send_sem=self.r['send'].at[self.w, k], recv_sem=self.r['pair_sem'].at[0],
                                         device_id={'cp': self.cp}, device_id_type=MESH).wait_send()

    @property
    def partner(self):
        return self.cp + 1 - 2 * self.core

    def pair_send(self):
        r, w = self.r, self.w
        self.send(r['sums'].at[w, 1 - self.core], r['pair'].at[w], r['pair_sem'].at[w], cp=self.partner)

    def pair_merge(self):
        r, w, rows = self.r, self.w, self.r['rows']
        self.wait(r['pair'].at[w], r['pair_sem'].at[w])
        for d in (2, 1, 3, 0):
            ox = lax.rem(self.x + d, self.n_x)
            merged, stat = merge_units([r['pair'][w, ox], r['sums'][w, self.core, ox]], rows, False)
            r['pair'][w, ox, pl.ds(0, rows), :] = merged
            r['pair'][w, ox, pl.ds(rows, STAT_ROWS), pl.ds(0, HEAD_DIM)] = stat
            if d:
                self.send(r['pair'].at[w, ox], r['xin'].at[w, d - 1], r['xin_sem'].at[w, d - 1], cp=self.cp_at(d))

    def project_out(self):
        r, w, rows = self.r, self.w, self.r['rows']
        for d in range(1, self.n_x):
            self.wait(r['xin'].at[w, d - 1], r['xin_sem'].at[w, d - 1])
        units = [r['pair'][w, self.x]] + [r['xin'][w, d - 1] for d in range(1, self.n_x)]
        attn, _ = merge_units(units, rows, True)
        attn = attn.astype(BF16)
        n_half = r['n_half']
        group = rows // n_half
        lhs = jnp.concatenate([attn[g * n_half:(g + 1) * n_half, k * HEAD_DIM:(k + 1) * HEAD_DIM] for k in range(2) for g in range(group)], axis=1)
        width = r['wo'].shape[1] // self.n_tp
        for d in (2, 1, 3, 0):
            oy = lax.rem(self.tp + d, self.n_tp)
            for part in range(0, width, 256):
                cols = pl.ds(pl.multiple_of(oy * width + part, 128), 256)
                r['yout'][w, oy, :, pl.ds(part, 256)] = jnp.dot(lhs, r['wo'][:, cols], preferred_element_type=F32)
            if d:
                self.send(r['yout'].at[w, oy], r['yin'].at[w, d - 1], r['yin_sem'].at[w, d - 1], tp=self.tp_at(d))

    def finish_rows(self):
        r, w = self.r, self.w
        for d in range(1, self.n_tp):
            self.wait(r['yin'].at[w, d - 1], r['yin_sem'].at[w, d - 1])
        width = r['wo'].shape[1] // self.n_tp
        n_half = r['n_half']
        total = r['yout'][w, self.tp]
        for d in range(1, self.n_tp):
            total = total + r['yin'][w, d - 1]
        row = pl.multiple_of((w * self.n_cp + self.cp) * n_half, n_half)
        cols = pl.ds(pl.multiple_of(self.tp * width, 128), width)
        total = total + r['x'][pl.ds(row, n_half), cols].astype(F32)
        r['gather'][w, self.cp, self.tp] = total.astype(BF16).astype(F32)

    def unit(self, half, rx, ry, sub=None):
        size = self.r['n_half'] // 2
        start = half * size
        if sub is not None:
            start, size = start + sub * (size // 2), size // 2
        return self.r['gather'].at[self.w, self.cp_at(rx), self.tp_at(ry), pl.ds(start, size), :]

    def hop(self, half, rx, ry, axis, step, sub=None):
        ref = self.unit(half, rx, ry, sub)
        tx, ty = (rx - step) % self.n_x, ry
        if axis == 'y':
            tx, ty = rx, (ry - step) % self.n_tp
        sem = self.r['gather_sem'].at[self.w, half, tx, ty, sub or 0]
        if axis == 'x':
            self.send(ref, ref, sem, cp=self.cp_at(step))
        else:
            self.send(ref, ref, sem, tp=self.tp_at(step))

    def arrive(self, half, rx, ry, sub=None):
        self.wait(self.unit(half, rx, ry, sub), self.r['gather_sem'].at[self.w, half, rx, ry, sub or 0])

    def share(self, half, rx, ry):
        ref = self.unit(half, rx, ry)
        self.send(ref, ref, self.r['share_sem'].at[self.w, half, rx, ry], cp=self.partner)

    def axes(self, half):
        return ('x', 'y') if half == 0 else ('y', 'x')

    def at(self, half, a, b):
        return (a, b) if half == 0 else (b, a)

    def gather_start(self):
        for half in (0, 1):
            for axis in self.axes(half):
                for step in (1, -1):
                    self.hop(half, 0, 0, axis, step)
        for half in (0, 1):
            self.share(half, 0, 0)

    def gather_first(self):
        for a, step in ((3, 1), (1, -1)):
            for half in (0, 1):
                one, two = self.axes(half)
                rx, ry = self.at(half, a, 0)
                self.arrive(half, rx, ry)
                self.hop(half, rx, ry, one, step, sub=0 if step == 1 else 1)
                self.hop(half, rx, ry, two, 1)
                self.hop(half, rx, ry, two, -1)
                self.share(half, rx, ry)

    def gather_opposite(self):
        for half in (0, 1):
            one, two = self.axes(half)
            rx, ry = self.at(half, 2, 0)
            self.arrive(half, rx, ry, 0)
            self.arrive(half, rx, ry, 1)
            self.hop(half, rx, ry, two, 1)
            self.hop(half, rx, ry, two, -1)
            self.share(half, rx, ry)

    def gather_second(self):
        for a in (0, 3, 1, 2):
            for b, step in ((3, 1), (1, -1)):
                for half in (0, 1):
                    one, two = self.axes(half)
                    rx, ry = self.at(half, a, b)
                    self.arrive(half, rx, ry)
                    self.hop(half, rx, ry, two, step, sub=0 if step == 1 else 1)
                    self.share(half, rx, ry)

    def gather_last(self):
        for a in (0, 3, 1, 2):
            for half in (0, 1):
                rx, ry = self.at(half, a, 2)
                self.arrive(half, rx, ry, 0)
                self.arrive(half, rx, ry, 1)
                self.share(half, rx, ry)

    def gather_shared(self):
        size = self.r['n_half'] // 2
        for half in (0, 1):
            for rx in range(self.n_x):
                for ry in range(self.n_tp):
                    cp = self.cp_at(rx) + 1 - 2 * self.core
                    ref = self.r['gather'].at[self.w, cp, self.tp_at(ry), pl.ds(half * size, size), :]
                    self.wait(ref, self.r['share_sem'].at[self.w, half, rx, ry])

    def out_copy(self, w):
        r = self.r
        n_rows = r['stage'].shape[1]
        return pltpu.make_async_copy(r['stage'].at[w % 2], r['out'].at[pl.ds(pl.multiple_of(w * n_rows, n_rows), n_rows), :], r['out_sem'].at[w % 2])

    def write_rows(self):
        r, w = self.r, self.w
        n_half = r['n_half']
        width = r['wo'].shape[1] // self.n_tp

        @pl.when(w >= 2)
        def _():
            self.out_copy(w - 2).wait()

        def body(s, carry):
            row = pl.ds(pl.multiple_of(s * n_half, n_half), n_half)
            for ty in range(self.n_tp):
                r['stage'][w % 2, row, pl.ds(ty * width, width)] = r['gather'][w, s, ty].astype(BF16)
            return carry
        lax.fori_loop(0, self.n_cp, body, 0)
        self.out_copy(w).start()


def entry_barrier(n_cp, n_tp):
    cp, tp = lax.axis_index('cp'), lax.axis_index('tp')
    barrier = pltpu.get_barrier_semaphore()
    peers = [{'cp': cp + 1 - 2 * (cp % 2)}]
    peers += [{'cp': lax.rem(cp + 2 * d, n_cp)} for d in range(1, n_cp // 2)]
    peers += [{'tp': lax.rem(tp + d, n_tp)} for d in range(1, n_tp)]
    for peer in peers:
        pl.semaphore_signal(barrier, inc=1, device_id=peer, device_id_type=MESH)
    pl.semaphore_wait(barrier, len(peers))


def project_block(block, r):
    n_rows = r['normed'].shape[0]
    base = pl.multiple_of(block * n_rows, n_rows)

    def norm_rows(t, carry):
        step = 32
        row = pl.multiple_of(t * step, step)
        x = r['x'][pl.ds(base + row, step), :].astype(F32)
        scale = lax.rsqrt(jnp.mean(jnp.square(x), axis=1, keepdims=True) + 1e-6)
        r['normed'][pl.ds(row, step), :] = (x * scale * r['gain'][...]).astype(BF16)
        return carry
    lax.fori_loop(0, n_rows // 32, norm_rows, 0)
    cos_t = r['rope'][pl.ds(base, n_rows), :HEAD_DIM]
    sin_t = r['rope'][pl.ds(base, n_rows), HEAD_DIM:]
    n_q = r['q'].shape[1] // HEAD_DIM

    def rotate(lin, gain):
        lin = lin.astype(BF16).astype(F32)
        lin = lin * lax.rsqrt(jnp.mean(jnp.square(lin), axis=1, keepdims=True) + 1e-6) * gain
        return lin * cos_t + pltpu.roll(lin, HEAD_DIM // 2, 1) * sin_t
    for pair in range(n_q // 2 + 2):
        lin = jnp.dot(r['normed'][...], r['w'][:, pl.ds(pair * 2 * HEAD_DIM, 2 * HEAD_DIM)], preferred_element_type=F32)
        for h in range(2):
            part = lin[:, h * HEAD_DIM:(h + 1) * HEAD_DIM]
            lanes = pl.ds(h * HEAD_DIM, HEAD_DIM)
            if pair < n_q // 2:
                r['q'][:, pl.ds((2 * pair + h) * HEAD_DIM, HEAD_DIM)] = rotate(part, r['q_norm'][...]).astype(BF16)
                continue
            name = 'k' if pair == n_q // 2 else 'v'
            part = rotate(part, r['k_norm'][...]) if name == 'k' else part
            part = part.astype(BF16)
            r[name][:, lanes] = part
            r['mix'][pl.ds(h, n_rows, stride=2), :] = part.astype(F32)
        if pair >= n_q // 2:
            name = 'k' if pair == n_q // 2 else 'v'
            rows = pl.ds(pl.multiple_of(2 * base, 2 * n_rows), 2 * n_rows)
            r[name + '_stage'][rows, :] = r['mix'][...].astype(BF16)
            pltpu.make_async_copy(r[name + '_stage'].at[rows, :], r[name + '_out'].at[rows, :], r['new_sem'].at[block, 0 if name == 'k' else 1]).start()


PHASES = (('pair_send', 3), ('pair_merge', 4), ('project_out', 6), ('finish_rows+gather_start', 8), ('gather_first', 9), ('gather_opposite', 10),
          ('gather_second', 12), ('gather_last', 14), ('gather_shared+write_rows', 15))


def block_kernel(n_cp, n_tp, len_ref, rope_hbm, gain_ref, qn_ref, kn_ref, x_hbm, wq_hbm, wk_hbm, wv_hbm, wo_hbm, k_hbm, v_hbm,
                 out_ref, kout_ref, vout_ref,
                 x_buf, w_buf, wo_buf, rope_buf, normed, q_buf, k_new, v_new, mix, k_stage, v_stage, k_buf, v_buf, score, even, odd,
                 sums, pair, xin, yout, yin, gather, stage,
                 load_sem, x_sem, k_sem, v_sem, new_sem, send_sem, pair_sem, xin_sem, yin_sem, gather_sem, share_sem, out_sem):
    n_seq, n_keys = k_hbm.shape[0], k_hbm.shape[1]
    n_waves = n_seq // WAVE_SEQS
    n_new = x_buf.shape[0] // n_seq
    wave_rows = WAVE_SEQS * n_new
    cp_index = lax.axis_index('cp')

    def kv_copies(i, slot):
        return (pltpu.make_async_copy(k_hbm.at[i], k_buf.at[slot], k_sem.at[slot]),
                pltpu.make_async_copy(v_hbm.at[i], v_buf.at[slot], v_sem.at[slot]))

    def x_copy(b):
        rows = pl.ds(b * wave_rows, wave_rows)
        return pltpu.make_async_copy(x_hbm.at[rows, :], x_buf.at[rows, :], x_sem.at[b])
    q_width, kv_width = wq_hbm.shape[1], wk_hbm.shape[1]
    loads = [pltpu.make_async_copy(rope_hbm, rope_buf, load_sem.at[0]),
             pltpu.make_async_copy(wq_hbm, w_buf.at[:, pl.ds(0, q_width)], load_sem.at[1]),
             pltpu.make_async_copy(wk_hbm, w_buf.at[:, pl.ds(q_width, kv_width)], load_sem.at[2]),
             pltpu.make_async_copy(wv_hbm, w_buf.at[:, pl.ds(q_width + kv_width, kv_width)], load_sem.at[3])]
    x_copy(0).start()
    for load in loads:
        load.start()
    for copy in kv_copies(0, 0):
        copy.start()
    for b in range(1, n_waves):
        x_copy(b).start()
    wo_load = pltpu.make_async_copy(wo_hbm, wo_buf, load_sem.at[4])
    wo_load.start()
    entry_barrier(n_cp, n_tp)
    parity = (lax.broadcasted_iota(jnp.int32, even.shape, 0) % 2).astype(F32)
    odd[...] = parity.astype(BF16)
    even[...] = (1.0 - parity).astype(BF16)
    for b in range(n_waves):
        if b == 0:
            x_copy(b).wait()
    for load in loads:
        load.wait()
    refs = {'x': x_buf, 'w': w_buf, 'wo': wo_buf, 'rope': rope_buf, 'gain': gain_ref, 'q_norm': qn_ref, 'k_norm': kn_ref, 'normed': normed,
            'q': q_buf, 'k': k_new, 'v': v_new, 'mix': mix, 'k_stage': k_stage, 'v_stage': v_stage, 'k_out': kout_ref, 'v_out': vout_ref,
            'new_sem': new_sem, 'sums': sums, 'pair': pair, 'xin': xin, 'yout': yout, 'yin': yin, 'gather': gather, 'stage': stage, 'out': out_ref,
            'send': send_sem, 'pair_sem': pair_sem, 'xin_sem': xin_sem, 'yin_sem': yin_sem, 'gather_sem': gather_sem, 'share_sem': share_sem,
            'out_sem': out_sem, 'rows': pair.shape[2] - STAT_ROWS, 'n_half': n_new // 2, 'sent': []}
    rows = refs['rows']

    def attention(i):
        wave, j, slot = i // WAVE_SEQS, i % WAVE_SEQS, i % 2

        @pl.when(i + 1 < n_seq)
        def _():
            for copy in kv_copies(i + 1, 1 - slot):
                copy.start()
        for copy in kv_copies(i, slot):
            copy.wait()
        limit = len_ref[i] - cp_index * (n_keys // 2)
        toks = pl.ds(pl.multiple_of(j * n_new, n_new), n_new)
        acc, stat = attend_seq(q_buf[toks, :], k_buf.at[slot], v_buf.at[slot], k_new[toks, :], v_new[toks, :], limit, cp_index == 0, score, even, odd)
        for h in range(2):
            sums[wave, h, j, pl.ds(0, rows), :] = acc[h * rows:(h + 1) * rows]
            sums[wave, h, j, pl.ds(rows, STAT_ROWS), pl.ds(0, HEAD_DIM)] = stat[:, h * HEAD_DIM:(h + 1) * HEAD_DIM]

    def step(i, carry):
        refs['sent'] = []

        @pl.when((i < n_seq) & (i % WAVE_SEQS == 0))
        def _():
            block = i // WAVE_SEQS

            @pl.when(block > 0)
            def _():
                rows_b = pl.ds(pl.multiple_of(block * wave_rows, wave_rows), wave_rows)
                pltpu.make_async_copy(x_hbm.at[rows_b, :], x_buf.at[rows_b, :], x_sem.at[block]).wait()
            project_block(block, refs)

        @pl.when(i < n_seq)
        def _():
            attention(i)

        @pl.when(i == WAVE_SEQS)
        def _():
            wo_load.wait()
        for name, delay in PHASES:
            at = i - delay

            @pl.when((at >= 0) & (at % WAVE_SEQS == 0) & (at < n_seq))
            def _(name=name, at=at):
                wave = Exchange(at // WAVE_SEQS, refs, n_cp, n_tp)
                for part in name.split('+'):
                    getattr(wave, part)()
        return carry
    lax.fori_loop(0, n_seq - WAVE_SEQS + PHASES[-1][1] + 1, step, 0)

    def drain(w, carry):
        wave = Exchange(w, refs, n_cp, n_tp)
        wave.wait_sends()
        rows_w = pl.ds(pl.multiple_of(2 * w * wave_rows, 2 * wave_rows), 2 * wave_rows)
        pltpu.make_async_copy(k_stage.at[rows_w, :], kout_ref.at[rows_w, :], new_sem.at[w, 0]).wait()
        pltpu.make_async_copy(v_stage.at[rows_w, :], vout_ref.at[rows_w, :], new_sem.at[w, 1]).wait()

        @pl.when(w >= n_waves - 2)
        def _():
            wave.out_copy(w).wait()
        return carry
    lax.fori_loop(0, n_waves, drain, 0)


def solution(mesh):
    n_cp, n_tp = mesh.shape['cp'], mesh.shape['tp']

    def per_device(hidden, prefix_len, k_cache, v_cache, attn_norm, w_q, w_k, w_v, w_o, q_norm, k_norm):
        n_seq, n_new, d_model = hidden.shape
        n_keys = k_cache.shape[1] * 2
        n_waves, n_x, n_half = n_seq // WAVE_SEQS, n_cp // 2, n_new // 2
        wave_rows = WAVE_SEQS * n_new
        q_width, kv_width = w_q.shape[1], w_k.shape[1]
        rows = n_half * q_width // (2 * HEAD_DIM)
        unit = (rows + STAT_ROWS, 2 * HEAD_DIM)
        width = d_model // n_tp
        chunk = min(512, n_keys)
        n_send = 1 + (n_x - 1) + (n_tp - 1) + 40 + 32
        vmem = pl.BlockSpec(memory_space=pltpu.VMEM)
        hbm = pl.BlockSpec(memory_space=pl.ANY)
        dma = pltpu.SemaphoreType.DMA
        block_out, k_new, v_new = pl.pallas_call(
            functools.partial(block_kernel, n_cp, n_tp),
            out_shape=(jax.ShapeDtypeStruct((n_seq * n_new, d_model), BF16), jax.ShapeDtypeStruct((n_seq * n_new * 2, HEAD_DIM), BF16),
                       jax.ShapeDtypeStruct((n_seq * n_new * 2, HEAD_DIM), BF16)),
            in_specs=[pl.BlockSpec(memory_space=pltpu.SMEM), hbm, vmem, vmem, vmem] + [hbm] * 7,
            out_specs=(hbm, hbm, hbm),
            scratch_shapes=[
                pltpu.VMEM((n_seq * n_new, d_model), BF16),
                pltpu.VMEM((d_model, q_width + 2 * kv_width), BF16),
                pltpu.VMEM((q_width, d_model), BF16),
                pltpu.VMEM((n_seq * n_new, 2 * HEAD_DIM), F32),
                pltpu.VMEM((wave_rows, d_model), BF16),
                pltpu.VMEM((wave_rows, q_width), BF16),
                pltpu.VMEM((wave_rows, kv_width), BF16),
                pltpu.VMEM((wave_rows, kv_width), BF16),
                pltpu.VMEM((2 * wave_rows, HEAD_DIM), F32),
                pltpu.VMEM((2 * n_seq * n_new, HEAD_DIM), BF16),
                pltpu.VMEM((2 * n_seq * n_new, HEAD_DIM), BF16),
                pltpu.VMEM((2, n_keys, HEAD_DIM), BF16),
                pltpu.VMEM((2, n_keys, HEAD_DIM), BF16),
                pltpu.VMEM((2 * rows, n_keys), F32),
                pltpu.VMEM((chunk, HEAD_DIM), BF16),
                pltpu.VMEM((chunk, HEAD_DIM), BF16),
                pltpu.VMEM((n_waves, 2, n_x) + unit, F32),
                pltpu.VMEM((n_waves, n_x) + unit, F32),
                pltpu.VMEM((n_waves, n_x - 1) + unit, F32),
                pltpu.VMEM((n_waves, n_tp, n_half, width), F32),
                pltpu.VMEM((n_waves, n_tp - 1, n_half, width), F32),
                pltpu.VMEM((n_waves, n_cp, n_tp, n_half, width), F32),
                pltpu.VMEM((2, wave_rows, d_model), BF16),
                dma((5,)), dma((n_waves,)), dma((2,)), dma((2,)), dma((n_waves, 2)), dma((n_waves, n_send)), dma((n_waves,)),
                dma((n_waves, n_x - 1)), dma((n_waves, n_tp - 1)), dma((n_waves, 2, n_x, n_tp, 2)), dma((n_waves, 2, n_x, n_tp)), dma((2,)),
            ],
            compiler_params=pltpu.CompilerParams(collective_id=0, has_side_effects=True, vmem_limit_bytes=67043328),
            name='block',
        )(prefix_len, rope_tables(prefix_len, n_new), attn_norm.astype(F32)[None], q_norm.astype(F32)[None], k_norm.astype(F32)[None],
          hidden.reshape(n_seq * n_new, d_model), w_q, w_k, w_v, w_o,
          k_cache.reshape(n_seq, n_keys, HEAD_DIM), v_cache.reshape(n_seq, n_keys, HEAD_DIM))
        new_shape = (n_seq, n_new, 2, HEAD_DIM)
        return block_out.reshape(n_seq, n_new, d_model), k_new.reshape(new_shape), v_new.reshape(new_shape)

    cache_spec = P('dp', 'cp', 'tp', None)
    arg_specs = (P('dp', None, None), P('dp'), cache_spec, cache_spec, P(None), P(None, 'tp'), P(None, 'tp'), P(None, 'tp'), P('tp', None), P(None), P(None))
    out_specs = (P('dp', None, None), P('dp', None, 'tp', None), P('dp', None, 'tp', None))
    return jax.shard_map(per_device, mesh=mesh, in_specs=arg_specs, out_specs=out_specs, check_vma=False)
```
